32 devices in a mesh: section: 4 (over x, core), head: 4 (over z), dp: 2 (over y).
Axes of the slice: x: 2, y: 2, z: 4, core: 2. Of those that a mesh axis runs over, the one named last changes fastest.
Arguments:
- teacher_q: bfloat16 [4, 256, 8192], P('section', 'dp', 'head'), may hold values from -150 to 150
- teacher_k: bfloat16 [4, 256, 1024], P('section', 'dp', 'head'), may hold values from -150 to 150
- student_q: bfloat16 [4, 2, 256, 4096], P('section', None, 'dp', 'head'), may hold values from -150 to 150
- student_k: bfloat16 [4, 2, 256, 1024], P('section', None, 'dp', 'head'), may hold values from -150 to 150
- student_scale: float32 [4, 32], P(None, 'head'), may hold values from 0.5 to 2
- pairing: int32 [4], replicated, may hold values from 0 to 3, as said below
- placement: int32 [4], replicated, may hold values from 0 to 3, as said below
Outputs:
- student_q_grad: bfloat16 [4, 2, 256, 4096], P('section', None, 'dp', 'head')
- student_k_grad: bfloat16 [4, 2, 256, 1024], P('section', None, 'dp', 'head')
- layer_kl: float32 [2, 4], P('dp')
- scale_grad: float32 [4, 32], P(None, 'head')
The draws below stay inside these ranges and needn't reach their ends.
Inputs may be any that keep to these rules, and one draw needn't show every extreme that they name: `pairing`: each teacher layer of the window is paired with exactly one student layer. `placement`: a section holds at most 2 student layers, in increasing order of layer index, and some section holds exactly 2.
All inputs are finite; a program needn't handle non-finite values.
Results may differ from the reference program's by a relative error of at most 0.0048.
Values may be sent and summed in bfloat16 or wider, within the bound.
A program may use at most 64 MiB of HBM per device.

```python
import math
import jax
import jax.numpy as jnp
from jax import lax

TH = 64
TKV = 8
STUDENT_HEADS = 32
STUDENT_KEY_HEADS = 8
HEAD_WIDTH = 128
REPLICA_TOKENS = 128
SECTION_SLOTS = 2
TLAYERS = 4
SLAYERS = 4
N_SECTION = 4
N_DP = 2


def matched_layer_pair(key, leading, kv_heads, per_group):
    key_query, key_keys = jax.random.split(key, 2)
    keys_all = jax.random.normal(key_keys, leading + (N_DP, REPLICA_TOKENS, kv_heads, HEAD_WIDTH), jnp.float32)
    queries = jax.random.normal(key_query, leading + (N_DP, REPLICA_TOKENS, kv_heads, per_group, HEAD_WIDTH), jnp.float32)
    queries = queries.reshape(leading + (N_DP * REPLICA_TOKENS, kv_heads * per_group * HEAD_WIDTH))
    keys_all = keys_all.reshape(leading + (N_DP * REPLICA_TOKENS, kv_heads * HEAD_WIDTH))
    return (queries, keys_all)


def teacher_pair(key):
    return matched_layer_pair(jax.random.fold_in(key, 11), (TLAYERS,), TKV, TH // TKV)


def student_pair(key):
    return matched_layer_pair(jax.random.fold_in(key, 23), (N_SECTION, SECTION_SLOTS), STUDENT_KEY_HEADS, STUDENT_HEADS // STUDENT_KEY_HEADS)


def draw_teacher_q(key, part):
    return teacher_pair(key)[0].astype(jnp.bfloat16)


def draw_teacher_k(key, part):
    return teacher_pair(key)[1].astype(jnp.bfloat16)


def draw_student_q(key, part):
    return student_pair(key)[0].astype(jnp.bfloat16)


def draw_student_k(key, part):
    return student_pair(key)[1].astype(jnp.bfloat16)


def layout_helper(key):
    key_heavy, key_slots, key_layers = jax.random.split(jax.random.fold_in(key, 37), 3)
    total_slots = N_SECTION * SECTION_SLOTS
    heavy = jax.random.randint(key_heavy, (), 0, N_SECTION).astype(jnp.int32)
    slot_order = jax.random.permutation(key_slots, total_slots).astype(jnp.int32)
    section_order = slot_order // SECTION_SLOTS
    priority = jnp.where(section_order == heavy, slot_order % SECTION_SLOTS - SECTION_SLOTS, jnp.arange(total_slots, dtype=jnp.int32))
    picked = jnp.argsort(priority, stable=True)[:SLAYERS]
    sections_taken = section_order[picked].astype(jnp.int32)
    layer_order = jax.random.permutation(key_layers, SLAYERS)
    placed = jnp.zeros((SLAYERS,), jnp.int32).at[layer_order].set(sections_taken)
    return (placed, heavy)


def force_value(order, layer_at, wanted):
    layer_ids = jnp.arange(SLAYERS, dtype=jnp.int32)
    holder = jnp.sum(jnp.where(order == wanted, layer_ids, 0)).astype(jnp.int32)
    current = jnp.sum(jnp.where(layer_ids == layer_at, order, 0)).astype(jnp.int32)
    order = jnp.where(layer_ids == holder, current, order)
    return jnp.where(layer_ids == layer_at, wanted, order).astype(jnp.int32)


def draw_placement(key, part):
    return layout_helper(key)[0]


def draw_pairing(key, part):
    placed, heavy = layout_helper(key)
    layer_ids = jnp.arange(SLAYERS, dtype=jnp.int32)
    order = jax.random.permutation(jax.random.fold_in(key, 53), TLAYERS).astype(jnp.int32)
    first_layer = jnp.min(jnp.where(placed == heavy, layer_ids, SLAYERS)).astype(jnp.int32)
    second_layer = jnp.max(jnp.where(placed == heavy, layer_ids, -1)).astype(jnp.int32)
    order = force_value(order, first_layer, (heavy + N_SECTION - 1) % N_SECTION)
    order = force_value(order, second_layer, (heavy + N_SECTION // 2) % N_SECTION)
    return order


def levels(key, dims, shards, low, top_value):
    factor_of = 1.0
    for dim, parts in shards:
        heights = jax.random.uniform(jax.random.fold_in(jax.random.fold_in(key, 6), dim), (parts,), jnp.float32, low / len(shards), top_value / len(shards))
        factor_of = factor_of * jnp.repeat(jnp.exp(heights), dims[dim] // parts).reshape((-1,) + (1,) * (len(dims) - 1 - dim))
    return factor_of


def setup_inputs(seed: int = 0) -> dict:
    key_of = jax.random.split(jax.random.key(seed), 8)
    teacher_q = draw_teacher_q(jax.random.fold_in(key_of[7], 71), 0)
    teacher_k = draw_teacher_k(jax.random.fold_in(key_of[7], 71), 0)
    student_q = draw_student_q(jax.random.fold_in(key_of[7], 71), 0)
    student_k = draw_student_k(jax.random.fold_in(key_of[7], 71), 0)
    student_scale = jnp.clip(jnp.exp(math.log(2.0) - 1.3862944 * jax.random.uniform(key_of[4], (SLAYERS, STUDENT_HEADS), jnp.float32) ** levels(key_of[4], (SLAYERS, STUDENT_HEADS), ((1, 4),), -0.2, 0.2)), 0.5, 2.0)
    pairing = draw_pairing(jax.random.fold_in(key_of[7], 71), 0)
    placement = draw_placement(jax.random.fold_in(key_of[7], 71), 0)
    return {"teacher_q": teacher_q, "teacher_k": teacher_k, "student_q": student_q, "student_k": student_k, "student_scale": student_scale, "pairing": pairing, "placement": placement}


def causal_mask(length):
    row_ids = lax.broadcasted_iota(jnp.int32, (length, length), 0)
    col_ids = lax.broadcasted_iota(jnp.int32, (length, length), 1)
    return col_ids <= row_ids

def head_terms(query_twins, teacher_key, query_head, student_key, scale_value, mask):
    width = teacher_key.shape[-1]
    inverse = 1.0 / math.sqrt(width)
    teacher_scores = jnp.einsum('hid,jd->hij', query_twins.astype(jnp.float32), teacher_key.astype(jnp.float32)) * inverse
    teacher_logp = jax.nn.log_softmax(jnp.where(mask, teacher_scores, -1e+30), axis=-1)
    target_logp = jnp.logaddexp(teacher_logp[0], teacher_logp[1]) - math.log(2.0)
    raw_scores = jnp.dot(query_head, student_key.T, preferred_element_type=jnp.float32) * inverse
    student_logp = jax.nn.log_softmax(jnp.where(mask, scale_value * raw_scores, -1e+30), axis=-1)
    target_prob = jnp.exp(target_logp)
    student_prob = jnp.exp(student_logp)
    divergence = jnp.sum(jnp.where(mask, target_prob * (target_logp - student_logp), 0.0))
    difference = jnp.where(mask, student_prob - target_prob, 0.0)
    scale_term = jnp.sum(difference * raw_scores)
    logit_grad = (difference * (scale_value * inverse)).astype(jnp.bfloat16)
    query_grad = jnp.dot(logit_grad, student_key, preferred_element_type=jnp.float32)
    key_grad = jnp.dot(logit_grad.T, query_head, preferred_element_type=jnp.float32)
    return (query_grad, key_grad, divergence, scale_term)

def group_terms(teacher_query, teacher_key, student_query, student_key, scales, mask):
    length = teacher_key.shape[0]
    width = teacher_key.shape[1]
    heads_here = scales.shape[0]
    teacher_heads = teacher_query.reshape(length, heads_here, 2, width).transpose(1, 2, 0, 3)
    student_heads = student_query.reshape(length, heads_here, width).transpose(1, 0, 2)

    def one_head(items):
        return head_terms(items[0], teacher_key, items[1], student_key, items[2], mask)
    query_grads, key_gradient_list, divergences, scale_terms = lax.map(one_head, (teacher_heads, student_heads, scales))
    query_grads = query_grads.transpose(1, 0, 2).reshape(length, heads_here * width)
    return (query_grads, lax.optimization_barrier(jnp.sum(key_gradient_list, 0)), jnp.sum(divergences), scale_terms)

def reference(teacher_q, teacher_k, student_q, student_k, student_scale, pairing, placement):
    mask = causal_mask(REPLICA_TOKENS)
    groups = TKV
    query_out = jnp.zeros(student_q.shape, jnp.bfloat16)
    key_out = jnp.zeros(student_k.shape, jnp.bfloat16)
    divergence_out = jnp.zeros((N_DP, SLAYERS), jnp.float32)
    scale_out = jnp.zeros((SLAYERS, STUDENT_HEADS), jnp.float32)
    layer_ids = jnp.arange(SLAYERS, dtype=jnp.int32)
    for layer in range(SLAYERS):
        section_of = placement[layer]
        slot_of = jnp.sum(((layer_ids < layer) & (placement == section_of)).astype(jnp.int32)).astype(jnp.int32)
        teacher_layer = pairing[layer]
        teacher_query_layer = teacher_q[teacher_layer]
        teacher_key_layer = teacher_k[teacher_layer]
        student_query_layer = student_q[section_of, slot_of]
        student_key_layer = student_k[section_of, slot_of]
        scales = student_scale[layer].reshape(groups, STUDENT_HEADS // groups)

        def split_rows(array, replica):
            rows = lax.dynamic_slice_in_dim(array, (replica * REPLICA_TOKENS).astype(jnp.int32), REPLICA_TOKENS, 0)
            return rows.reshape(REPLICA_TOKENS, groups, -1).transpose(1, 0, 2)

        def replica_terms(replica):
            items = (split_rows(teacher_query_layer, replica), split_rows(teacher_key_layer, replica), split_rows(student_query_layer, replica), split_rows(student_key_layer, replica), scales)

            def group_call(group_items):
                return group_terms(group_items[0], group_items[1], group_items[2], group_items[3], group_items[4], mask)
            return lax.map(group_call, items)
        query_grads, key_gradient_list, divergences, scale_terms = lax.map(replica_terms, jnp.arange(N_DP, dtype=jnp.int32))
        query_grads = query_grads.transpose(0, 2, 1, 3).reshape(N_DP * REPLICA_TOKENS, STUDENT_HEADS * HEAD_WIDTH)
        key_gradient_list = key_gradient_list.transpose(0, 2, 1, 3).reshape(N_DP * REPLICA_TOKENS, STUDENT_KEY_HEADS * HEAD_WIDTH)
        query_out = query_out.at[section_of, slot_of].set(query_grads.astype(jnp.bfloat16))
        key_out = key_out.at[section_of, slot_of].set(key_gradient_list.astype(jnp.bfloat16))
        divergence_out = divergence_out.at[:, layer].set(lax.optimization_barrier(jnp.sum(divergences, 1)) / (STUDENT_HEADS * REPLICA_TOKENS))
        scale_out = scale_out.at[layer].set(lax.optimization_barrier(jnp.sum(scale_terms, 0)).reshape(STUDENT_HEADS))
    return (query_out, key_out, divergence_out, scale_out)
```

```python
import functools
import math

import jax
import jax.numpy as jnp
from jax import lax
from jax.experimental import pallas as pl
from jax.experimental.pallas import tpu as pltpu
from jax.sharding import PartitionSpec as P

WIDTH = 128
NEG = -1e30
TINY = 1.2e-38


def kernel(
    dims,
    pairing,
    placement,
    scale,
    tq_hbm,
    tk_hbm,
    sq_hbm,
    sk_hbm,
    qg_hbm,
    kg_hbm,
    kl_ref,
    sg_ref,
    tq,
    tk,
    sq,
    sk,
    qg,
    kg,
    p_s,
    lp_s,
    g_s,
    rows_s,
    red1,
    red_dp,
    red_head,
    in_sem,
    out_sem,
    x_send,
    x_recv,
    s_send,
    s_recv,
    r1_send,
    r1_recv,
    rd_send,
    rd_recv,
    rh_send,
    rh_recv,
    *gathered,
):
    n, n_head, n_dp, tokens, heads, groups, slots, layers = dims
    chunks = heads // 2
    per_group = heads // groups
    inverse = 1.0 / math.sqrt(WIDTH)
    me = lax.axis_index("section")
    my_head = lax.axis_index("head")
    my_dp = lax.axis_index("dp")
    half = n // 2
    sibling = me + 1 - 2 * lax.rem(me, 2)

    def lanes(index):
        return slice(index * WIDTH, (index + 1) * WIDTH)

    loads_t = [pltpu.make_async_copy(tk_hbm.at[0], tk, in_sem.at[0])]
    for c in range(chunks):
        part = slice(c * 4 * WIDTH, (c + 1) * 4 * WIDTH)
        loads_t.append(
            pltpu.make_async_copy(tq_hbm.at[0, :, part], tq.at[:, part], in_sem.at[3 + c])
        )
    loads_s = [
        pltpu.make_async_copy(sk_hbm.at[0], sk, in_sem.at[1]),
        pltpu.make_async_copy(sq_hbm.at[0], sq, in_sem.at[2]),
    ]
    for copy in loads_t + loads_s:
        copy.start()

    barrier = pltpu.get_barrier_semaphore()
    peers = 0
    for axis, mine, size in (("section", me, n), ("head", my_head, n_head), ("dp", my_dp, n_dp)):
        for k in range(1, size):
            pl.semaphore_signal(
                barrier,
                inc=1,
                device_id={axis: lax.rem(mine + k, size)},
                device_id_type=pl.DeviceIdType.MESH,
            )
            peers += 1

    def remote(src, dst, send, recv, axis, peer):
        return pltpu.make_async_remote_copy(
            src_ref=src,
            dst_ref=dst,
            send_sem=send,
            recv_sem=recv,
            device_id={axis: peer},
            device_id_type=pl.DeviceIdType.MESH,
        )

    key_ids = lax.broadcasted_iota(jnp.int32, (tokens, tokens), 0)
    query_ids = lax.broadcasted_iota(jnp.int32, (tokens, tokens), 1)
    visible = key_ids <= query_ids
    strict = key_ids < query_ids
    eye = key_ids == query_ids

    count = jnp.int32(0)
    slot_layer = [jnp.int32(0)] * slots
    slot_teacher = [jnp.int32(0)] * slots
    taught = jnp.int32(0)
    for l in range(layers):
        held = placement[l] == me
        for j in range(slots):
            here = held & (count == j)
            slot_layer[j] = jnp.where(here, l, slot_layer[j])
            slot_teacher[j] = jnp.where(here, pairing[l], slot_teacher[j])
        count = count + held.astype(jnp.int32)
        taught = jnp.where(pairing[l] == me, l, taught)
    slot_valid = [count > j for j in range(slots)]

    def nt(a, b):
        return lax.dot_general(a, b, (((1,), (1,)), ((), ())), preferred_element_type=jnp.float32)

    def target(key, b):
        total = None
        for a in (2 * b, 2 * b + 1):
            s = jnp.where(visible, nt(key, tq[:, lanes(a)]) * inverse, NEG)
            e = jnp.exp(s - jnp.max(s, axis=0, keepdims=True))
            p = e * (0.5 / jnp.sum(e, axis=0, keepdims=True))
            total = p if total is None else total + p
        return total

    entropy = jnp.zeros((1, tokens), jnp.float32)
    x_copies, s_copies = [], []
    loads_t[0].wait()
    for c in range(chunks):
        loads_t[1 + c].wait()
        buffer = gathered[c]
        b = 2 * c
        first = target(tk[:, lanes(b // per_group)], b)
        second = target(tk[:, lanes((b + 1) // per_group)], b + 1)
        buffer[me, :tokens, :] = jnp.where(visible, first, second.T)
        diagonal = jnp.sum(jnp.where(eye, second, 0.0), axis=0, keepdims=True)
        buffer[me, tokens:, :] = jnp.broadcast_to(diagonal, (8, tokens))
        for t in (first, second):
            entropy = entropy + jnp.sum(t * jnp.log(jnp.maximum(t, TINY)), axis=0, keepdims=True)
        if c == 0:
            pl.semaphore_wait(barrier, peers)
        mine = buffer.at[me]
        for k in range(1, half):
            copy = remote(
                mine, mine, x_send.at[c, k], x_recv.at[c, k], "section", lax.rem(me + 2 * k, n)
            )
            copy.start()
            x_copies.append(copy)
        copy = remote(mine, mine, s_send.at[c, 0], s_recv.at[c, 0], "section", sibling)
        copy.start()
        s_copies.append(copy)

    def student(j, b):
        value = scale[slot_layer[j], b]
        raw = nt(sk[j, :, lanes(b // per_group)], sq[j, :, lanes(b)])
        z = jnp.where(visible, raw * (value * inverse), NEG)
        z = z - jnp.max(z, axis=0, keepdims=True)
        e = jnp.exp(z)
        l = jnp.sum(e, axis=0, keepdims=True)
        logp = z - jnp.log(l)
        p = e * (1.0 / l)
        p_s[j, b] = p
        lp_s[j, b] = logp
        rows_s[j * heads + b] = jnp.sum(p * logp, axis=0, keepdims=True)

    for copy in loads_s:
        copy.wait()
    for c in range(chunks):
        for j in range(slots):
            for b in (2 * c, 2 * c + 1):
                student(j, b)
        for k in range(1, half):
            x_copies[c * (half - 1) + k - 1].wait_recv()
            block = gathered[c].at[lax.rem(me + n - 2 * k, n)]
            copy = remote(block, block, s_send.at[c, k], s_recv.at[c, k], "section", sibling)
            copy.start()
            s_copies.append(copy)

    cross = [jnp.zeros((1, tokens), jnp.float32)] * slots
    scale_rows = [[None] * heads for _ in range(slots)]
    for c in range(chunks):
        for k in range(half):
            index = c if k == 0 else chunks + c * (half - 1) + k - 1
            s_copies[index].wait_recv()
        for j in range(slots):
            packed = gathered[c][slot_teacher[j], :tokens, :]
            diagonal = gathered[c][slot_teacher[j], tokens : tokens + 1, :]
            for b in (2 * c, 2 * c + 1):
                if b == 2 * c:
                    t = jnp.where(visible, packed, 0.0)
                else:
                    t = jnp.where(strict, packed.T, jnp.where(eye, diagonal, 0.0))
                value = scale[slot_layer[j], b]
                row = jnp.sum(t * lp_s[j, b], axis=0, keepdims=True)
                cross[j] = cross[j] + row
                scale_rows[j][b] = (rows_s[j * heads + b] - row) / value
                factor = jnp.where(slot_valid[j], value * inverse, 0.0)
                g_s[j, b] = ((p_s[j, b] - t) * factor).astype(jnp.bfloat16)

    tile_rows = red1.shape[1]
    row_ids = lax.broadcasted_iota(jnp.int32, (tile_rows, WIDTH), 0)
    lane_ids = lax.broadcasted_iota(jnp.int32, (tile_rows, WIDTH), 1)
    tile = jnp.where(
        (row_ids == taught) & (lane_ids == heads), jnp.sum(entropy, axis=1, keepdims=True), 0.0
    )
    for j in range(slots):
        line = jnp.where(lane_ids == heads, -jnp.sum(cross[j], axis=1, keepdims=True), 0.0)
        for b in range(heads):
            line = jnp.where(
                lane_ids == b, jnp.sum(scale_rows[j][b], axis=1, keepdims=True), line
            )
        owner = jnp.where(slot_valid[j], slot_layer[j], -1)
        tile = tile + jnp.where(row_ids == owner, line, 0.0)
    red1[me] = tile
    r1_copies = []
    for k in range(1, n):
        mine = red1.at[me]
        copy = remote(mine, mine, r1_send.at[k], r1_recv.at[k], "section", lax.rem(me + k, n))
        copy.start()
        r1_copies.append(copy)

    def gradients(j, g):
        key = sk[j, :, lanes(g)]
        total = None
        for b in range(g * per_group, (g + 1) * per_group):
            grad = g_s[j, b]
            qg[j, :, lanes(b)] = lax.dot_general(
                grad, key, (((0,), (0,)), ((), ())), preferred_element_type=jnp.float32
            ).astype(jnp.bfloat16)
            term = jnp.dot(grad, sq[j, :, lanes(b)], preferred_element_type=jnp.float32)
            total = term if total is None else total + term
        kg[j, :, lanes(g)] = total.astype(jnp.bfloat16)
        part = slice(g * per_group * WIDTH, (g + 1) * per_group * WIDTH)
        copies = [
            pltpu.make_async_copy(
                qg.at[j, :, part], qg_hbm.at[0, j, :, part], out_sem.at[0, j, g]
            ),
            pltpu.make_async_copy(
                kg.at[j, :, lanes(g)], kg_hbm.at[0, j, :, lanes(g)], out_sem.at[1, j, g]
            ),
        ]
        for copy in copies:
            copy.start()
        return copies

    units = [(j, g) for j in range(slots) for g in range(groups)]
    out_copies = []
    for unit in units[: len(units) // 2]:
        out_copies += gradients(*unit)

    for copy in r1_copies:
        copy.wait_recv()
    tile = red1[0]
    for s in range(1, n):
        tile = tile + red1[s]
    red_dp[my_dp] = tile
    red_head[my_head] = tile
    r2_copies = []
    for axis, mine, size, buffer, send, recv in (
        ("head", my_head, n_head, red_head, rh_send, rh_recv),
        ("dp", my_dp, n_dp, red_dp, rd_send, rd_recv),
    ):
        for k in range(1, size):
            block = buffer.at[mine]
            copy = remote(block, block, send.at[k], recv.at[k], axis, lax.rem(mine + k, size))
            copy.start()
            r2_copies.append(copy)

    for unit in units[len(units) // 2 :]:
        out_copies += gradients(*unit)

    for copy in r2_copies:
        copy.wait_recv()
    tile = red_dp[0]
    for s in range(1, n_dp):
        tile = tile + red_dp[s]
    sg_ref[...] = tile[:layers, :heads]
    tile = red_head[0]
    for s in range(1, n_head):
        tile = tile + red_head[s]
    column = jnp.sum(jnp.where(lane_ids == heads, tile, 0.0), axis=1, keepdims=True)
    line = jnp.sum(jnp.where(row_ids == lane_ids, column, 0.0), axis=0, keepdims=True)
    kl_ref[...] = (line / (heads * n_head * tokens))[:, :layers]

    for copy in x_copies + s_copies + r1_copies + r2_copies:
        copy.wait_send()
    for copy in out_copies:
        copy.wait()


def local(n, n_head, n_dp, teacher_q, teacher_k, student_q, student_k, student_scale, pairing, placement):
    layers, heads = student_scale.shape
    slots, tokens = student_q.shape[1:3]
    groups = student_k.shape[3] // WIDTH
    chunks = heads // 2
    tile_rows = -(-layers // 8) * 8
    dims = (n, n_head, n_dp, tokens, heads, groups, slots, layers)
    smem = pl.BlockSpec(memory_space=pltpu.SMEM)
    hbm = pl.BlockSpec(memory_space=pl.ANY)
    vmem = pl.BlockSpec(memory_space=pltpu.VMEM)
    dma = pltpu.SemaphoreType.DMA
    f32, bf16 = jnp.float32, jnp.bfloat16
    return pl.pallas_call(
        functools.partial(kernel, dims),
        out_shape=(
            jax.ShapeDtypeStruct(student_q.shape, bf16),
            jax.ShapeDtypeStruct(student_k.shape, bf16),
            jax.ShapeDtypeStruct((1, layers), f32),
            jax.ShapeDtypeStruct((layers, heads), f32),
        ),
        in_specs=[smem, smem, smem, hbm, hbm, hbm, hbm],
        out_specs=(hbm, hbm, vmem, vmem),
        scratch_shapes=[
            pltpu.VMEM(teacher_q.shape[1:], bf16),
            pltpu.VMEM(teacher_k.shape[1:], bf16),
            pltpu.VMEM(student_q.shape[1:], bf16),
            pltpu.VMEM(student_k.shape[1:], bf16),
            pltpu.VMEM(student_q.shape[1:], bf16),
            pltpu.VMEM(student_k.shape[1:], bf16),
            pltpu.VMEM((slots, heads, tokens, tokens), f32),
            pltpu.VMEM((slots, heads, tokens, tokens), f32),
            pltpu.VMEM((slots, heads, tokens, tokens), bf16),
            pltpu.VMEM((slots * heads, 1, tokens), f32),
            pltpu.VMEM((n, tile_rows, WIDTH), f32),
            pltpu.VMEM((n_dp, tile_rows, WIDTH), f32),
            pltpu.VMEM((n_head, tile_rows, WIDTH), f32),
            dma((3 + chunks,)),
            dma((2, slots, groups)),
            dma((chunks, n // 2)),
            dma((chunks, n // 2)),
            dma((chunks, n // 2)),
            dma((chunks, n // 2)),
            dma((n,)),
            dma((n,)),
            dma((n_dp,)),
            dma((n_dp,)),
            dma((n_head,)),
            dma((n_head,)),
        ]
        + [pltpu.VMEM((n, tokens + 8, tokens), f32) for _ in range(chunks)],
        compiler_params=pltpu.CompilerParams(collective_id=0, has_side_effects=True),
    )(pairing, placement, student_scale, teacher_q, teacher_k, student_q, student_k)


def solution(mesh):
    sizes = (mesh.shape["section"], mesh.shape["head"], mesh.shape["dp"])
    return jax.shard_map(
        functools.partial(local, *sizes),
        mesh=mesh,
        in_specs=(
            P("section", "dp", "head"),
            P("section", "dp", "head"),
            P("section", None, "dp", "head"),
            P("section", None, "dp", "head"),
            P(None, "head"),
            P(),
            P(),
        ),
        out_specs=(
            P("section", None, "dp", "head"),
            P("section", None, "dp", "head"),
            P("dp", None),
            P(None, "head"),
        ),
        check_vma=False,
    )
```

```python
import functools
import math

import jax
import jax.numpy as jnp
from jax import lax
from jax.experimental import pallas as pl
from jax.experimental.pallas import tpu as pltpu
from jax.sharding import PartitionSpec as P

WIDTH = 128
NEG = -1e30
TINY = 1.2e-38


def kernel(
    dims,
    pairing,
    placement,
    scale,
    tq_hbm,
    tk_hbm,
    sq_hbm,
    sk_hbm,
    qg,
    kg,
    kl_ref,
    sg_ref,
    tq,
    tk,
    sq,
    sk,
    p_s,
    lp_s,
    g_s,
    rows_s,
    red_dp,
    red_head,
    in_sem,
    x_send,
    x_recv,
    s_send,
    s_recv,
    rd_send,
    rd_recv,
    rh_send,
    rh_recv,
    *gathered,
):
    n, n_head, n_dp, tokens, heads, groups, slots, layers = dims
    chunks = heads // 2
    per_group = heads // groups
    inverse = 1.0 / math.sqrt(WIDTH)
    me = lax.axis_index("section")
    my_head = lax.axis_index("head")
    my_dp = lax.axis_index("dp")
    half = n // 2
    sibling = me + 1 - 2 * lax.rem(me, 2)

    def lanes(index):
        return slice(index * WIDTH, (index + 1) * WIDTH)

    loads_t = [pltpu.make_async_copy(tk_hbm.at[0], tk, in_sem.at[0])]
    for c in range(chunks):
        part = slice(c * 4 * WIDTH, (c + 1) * 4 * WIDTH)
        loads_t.append(
            pltpu.make_async_copy(tq_hbm.at[0, :, part], tq.at[:, part], in_sem.at[3 + c])
        )
    loads_s = [
        pltpu.make_async_copy(sk_hbm.at[0], sk, in_sem.at[1]),
        pltpu.make_async_copy(sq_hbm.at[0], sq, in_sem.at[2]),
    ]
    for copy in loads_t + loads_s:
        copy.start()

    barrier = pltpu.get_barrier_semaphore()
    dp_peers = [
        ({"section": lax.rem(me + k, n), "dp": lax.rem(my_dp + d, n_dp)}, (k, d))
        for d in range(n_dp)
        for k in range(n)
        if (k, d) != (0, 0)
    ]
    head_peers = [
        ({"section": lax.rem(me + k, n), "head": lax.rem(my_head + h, n_head)}, (k, h))
        for h in range(1, n_head)
        for k in range(n)
    ]
    for peer, _ in dp_peers + head_peers:
        pl.semaphore_signal(barrier, inc=1, device_id=peer, device_id_type=pl.DeviceIdType.MESH)
    peers = len(dp_peers) + len(head_peers)

    def send(src, dst, send_sem, recv_sem, peer):
        return pltpu.make_async_remote_copy(
            src_ref=src,
            dst_ref=dst,
            send_sem=send_sem,
            recv_sem=recv_sem,
            device_id=peer,
            device_id_type=pl.DeviceIdType.MESH,
        )

    def remote(src, dst, send_sem, recv_sem, peer):
        return send(src, dst, send_sem, recv_sem, {"section": peer})

    key_ids = lax.broadcasted_iota(jnp.int32, (tokens, tokens), 0)
    query_ids = lax.broadcasted_iota(jnp.int32, (tokens, tokens), 1)
    visible = key_ids <= query_ids
    strict = key_ids < query_ids
    eye = key_ids == query_ids

    count = jnp.int32(0)
    slot_layer = [jnp.int32(0)] * slots
    slot_teacher = [jnp.int32(0)] * slots
    taught = jnp.int32(0)
    for l in range(layers):
        held = placement[l] == me
        for j in range(slots):
            here = held & (count == j)
            slot_layer[j] = jnp.where(here, l, slot_layer[j])
            slot_teacher[j] = jnp.where(here, pairing[l], slot_teacher[j])
        count = count + held.astype(jnp.int32)
        taught = jnp.where(pairing[l] == me, l, taught)
    slot_valid = [count > j for j in range(slots)]

    def nt(a, b):
        return lax.dot_general(a, b, (((1,), (1,)), ((), ())), preferred_element_type=jnp.float32)

    def target(key, b):
        total = None
        for a in (2 * b, 2 * b + 1):
            s = jnp.where(visible, nt(key, tq[:, lanes(a)]) * inverse, NEG)
            e = jnp.exp(s - jnp.max(s, axis=0, keepdims=True))
            p = e * (0.5 / jnp.sum(e, axis=0, keepdims=True))
            total = p if total is None else total + p
        return total

    entropy = jnp.zeros((1, tokens), jnp.float32)
    x_copies, s_copies = [], []
    loads_t[0].wait()
    for c in range(chunks):
        loads_t[1 + c].wait()
        buffer = gathered[c]
        b = 2 * c
        first = target(tk[:, lanes(b // per_group)], b)
        second = target(tk[:, lanes((b + 1) // per_group)], b + 1)
        buffer[me, :tokens, :] = jnp.where(visible, first, second.T)
        diagonal = jnp.sum(jnp.where(eye, second, 0.0), axis=0, keepdims=True)
        buffer[me, tokens:, :] = jnp.broadcast_to(diagonal, (8, tokens))
        for t in (first, second):
            entropy = entropy + jnp.sum(t * jnp.log(jnp.maximum(t, TINY)), axis=0, keepdims=True)
        if c == 0:
            pl.semaphore_wait(barrier, peers)
        mine = buffer.at[me]
        for k in range(1, half):
            copy = remote(
                mine, mine, x_send.at[c, k], x_recv.at[c, k], lax.rem(me + 2 * k, n)
            )
            copy.start()
            x_copies.append(copy)
        copy = remote(mine, mine, s_send.at[c, 0], s_recv.at[c, 0], sibling)
        copy.start()
        s_copies.append(copy)

    def student(j, b):
        value = scale[slot_layer[j], b]
        raw = nt(sk[j, :, lanes(b // per_group)], sq[j, :, lanes(b)])
        z = jnp.where(visible, raw * (value * inverse), NEG)
        z = z - jnp.max(z, axis=0, keepdims=True)
        e = jnp.exp(z)
        l = jnp.sum(e, axis=0, keepdims=True)
        logp = z - jnp.log(l)
        p = e * (1.0 / l)
        p_s[j, b] = p
        lp_s[j, b] = logp
        rows_s[j, b : b + 1, :] = jnp.sum(p * logp, axis=0, keepdims=True)

    cross = [jnp.zeros((1, tokens), jnp.float32)] * slots

    def compare(c):
        for k in range(half):
            index = c if k == 0 else chunks + c * (half - 1) + k - 1
            s_copies[index].wait_recv()
        for j in range(slots):
            packed = gathered[c][slot_teacher[j], :tokens, :]
            diagonal = gathered[c][slot_teacher[j], tokens : tokens + 1, :]
            for b in (2 * c, 2 * c + 1):
                if b == 2 * c:
                    t = jnp.where(visible, packed, 0.0)
                else:
                    t = jnp.where(strict, packed.T, jnp.where(eye, diagonal, 0.0))
                value = scale[slot_layer[j], b]
                row = jnp.sum(t * lp_s[j, b], axis=0, keepdims=True)
                cross[j] = cross[j] + row
                spot = slice(b, b + 1)
                rows_s[j, spot, :] = (rows_s[j, spot, :] - row) / value
                factor = jnp.where(slot_valid[j], value * inverse, 0.0)
                g_s[j, b] = ((p_s[j, b] - t) * factor).astype(jnp.bfloat16)

    def gradients(j, g):
        key = sk[j, :, lanes(g)]
        total = None
        for b in range(g * per_group, (g + 1) * per_group):
            grad = g_s[j, b]
            qg[0, j, :, lanes(b)] = lax.dot_general(
                grad, key, (((0,), (0,)), ((), ())), preferred_element_type=jnp.float32
            ).astype(jnp.bfloat16)
            term = jnp.dot(grad, sq[j, :, lanes(b)], preferred_element_type=jnp.float32)
            total = term if total is None else total + term
        kg[0, j, :, lanes(g)] = total.astype(jnp.bfloat16)

    ready = 0

    def finished_groups(heads_done, first):
        last = heads_done // per_group
        for g in range(first, last):
            for j in range(slots):
                gradients(j, g)
        return last

    for copy in loads_s:
        copy.wait()
    for c in range(chunks):
        for j in range(slots):
            for b in (2 * c, 2 * c + 1):
                student(j, b)
        for k in range(1, half):
            x_copies[c * (half - 1) + k - 1].wait_recv()
            block = gathered[c].at[lax.rem(me + n - 2 * k, n)]
            copy = remote(block, block, s_send.at[c, k], s_recv.at[c, k], sibling)
            copy.start()
            s_copies.append(copy)
        if c > 0:
            ready = finished_groups(2 * (c - 1), ready)
            compare(c - 1)
    ready = finished_groups(2 * (chunks - 1), ready)
    compare(chunks - 1)

    tile_rows = red_dp.shape[2]
    row_ids = lax.broadcasted_iota(jnp.int32, (tile_rows, WIDTH), 0)
    lane_ids = lax.broadcasted_iota(jnp.int32, (tile_rows, WIDTH), 1)
    head_rows = lax.broadcasted_iota(jnp.int32, (heads, WIDTH), 0)
    head_lanes = lax.broadcasted_iota(jnp.int32, (heads, WIDTH), 1)
    tile = jnp.where(
        (row_ids == taught) & (lane_ids == heads), jnp.sum(entropy, axis=1, keepdims=True), 0.0
    )
    for j in range(slots):
        column = jnp.sum(rows_s[j], axis=1, keepdims=True)
        line = jnp.sum(jnp.where(head_rows == head_lanes, column, 0.0), axis=0, keepdims=True)
        line = jnp.where(lane_ids == heads, -jnp.sum(cross[j], axis=1, keepdims=True), line)
        owner = jnp.where(slot_valid[j], slot_layer[j], -1)
        tile = tile + jnp.where(row_ids == owner, line, 0.0)
    red_dp[me, my_dp] = tile
    mine = red_dp.at[me, my_dp]
    r_copies = []
    for peer, (k, h) in head_peers:
        r_copies.append(
            send(mine, red_head.at[me, my_head], rh_send.at[k, h], rh_recv.at[k, h], peer)
        )
    for peer, (k, d) in dp_peers:
        r_copies.append(send(mine, mine, rd_send.at[k, d], rd_recv.at[k, d], peer))
    for copy in r_copies:
        copy.start()

    finished_groups(heads, ready)

    for copy in r_copies:
        copy.wait_recv()
    for s in range(n):
        red_head[s, my_head] = red_dp[s, my_dp]

    def added(buffer, size):
        total = None
        for a in range(size):
            for s in range(n):
                total = buffer[s, a] if total is None else total + buffer[s, a]
        return total

    sg_ref[...] = added(red_dp, n_dp)[:layers, :heads]
    column = jnp.sum(
        jnp.where(lane_ids == heads, added(red_head, n_head), 0.0), axis=1, keepdims=True
    )
    line = jnp.sum(jnp.where(row_ids == lane_ids, column, 0.0), axis=0, keepdims=True)
    kl_ref[...] = (line / (heads * n_head * tokens))[:, :layers]

    for copy in x_copies + s_copies + r_copies:
        copy.wait_send()


def hand_out(*refs):
    count = len(refs) // 2
    sems = refs[-1]
    copies = [
        pltpu.make_async_copy(refs[i], refs[count + i], sems.at[i]) for i in range(count)
    ]
    for copy in copies:
        copy.start()
    for copy in copies:
        copy.wait()


def local(n, n_head, n_dp, teacher_q, teacher_k, student_q, student_k, student_scale, pairing, placement):
    layers, heads = student_scale.shape
    slots, tokens = student_q.shape[1:3]
    groups = student_k.shape[3] // WIDTH
    chunks = heads // 2
    tile_rows = -(-layers // 8) * 8
    dims = (n, n_head, n_dp, tokens, heads, groups, slots, layers)
    smem = pl.BlockSpec(memory_space=pltpu.SMEM)
    hbm = pl.BlockSpec(memory_space=pltpu.HBM)
    vmem = pl.BlockSpec(memory_space=pltpu.VMEM)
    dma = pltpu.SemaphoreType.DMA
    f32, bf16 = jnp.float32, jnp.bfloat16
    shapes = (
        (student_q.shape, bf16),
        (student_k.shape, bf16),
        ((1, layers), f32),
        ((layers, heads), f32),
    )
    results = pl.pallas_call(
        functools.partial(kernel, dims),
        out_shape=tuple(pltpu.VMEM(*shape) for shape in shapes),
        in_specs=[smem, smem, smem, hbm, hbm, hbm, hbm],
        out_specs=(vmem,) * 4,
        scratch_shapes=[
            pltpu.VMEM(teacher_q.shape[1:], bf16),
            pltpu.VMEM(teacher_k.shape[1:], bf16),
            pltpu.VMEM(student_q.shape[1:], bf16),
            pltpu.VMEM(student_k.shape[1:], bf16),
            pltpu.VMEM((slots, heads, tokens, tokens), f32),
            pltpu.VMEM((slots, heads, tokens, tokens), f32),
            pltpu.VMEM((slots, heads, tokens, tokens), bf16),
            pltpu.VMEM((slots, heads, tokens), f32),
            pltpu.VMEM((n, n_dp, tile_rows, WIDTH), f32),
            pltpu.VMEM((n, n_head, tile_rows, WIDTH), f32),
            dma((3 + chunks,)),
            dma((chunks, n // 2)),
            dma((chunks, n // 2)),
            dma((chunks, n // 2)),
            dma((chunks, n // 2)),
            dma((n, n_dp)),
            dma((n, n_dp)),
            dma((n, n_head)),
            dma((n, n_head)),
        ]
        + [pltpu.VMEM((n, tokens + 8, tokens), f32) for _ in range(chunks)],
        compiler_params=pltpu.CompilerParams(
            collective_id=0, has_side_effects=True, vmem_limit_bytes=56 * 1024 * 1024
        ),
    )(pairing, placement, student_scale, teacher_q, teacher_k, student_q, student_k)
    return pl.pallas_call(
        hand_out,
        out_shape=tuple(jax.ShapeDtypeStruct(*shape) for shape in shapes),
        in_specs=[vmem] * 4,
        out_specs=(hbm,) * 4,
        scratch_shapes=[dma((4,))],
        compiler_params=pltpu.CompilerParams(vmem_limit_bytes=4 * 1024 * 1024),
    )(*results)


def solution(mesh):
    sizes = (mesh.shape["section"], mesh.shape["head"], mesh.shape["dp"])
    return jax.shard_map(
        functools.partial(local, *sizes),
        mesh=mesh,
        in_specs=(
            P("section", "dp", "head"),
            P("section", "dp", "head"),
            P("section", None, "dp", "head"),
            P("section", None, "dp", "head"),
            P(None, "head"),
            P(),
            P(),
        ),
        out_specs=(
            P("section", None, "dp", "head"),
            P("section", None, "dp", "head"),
            P("dp", None),
            P(None, "head"),
        ),
        check_vma=False,
    )
```

```python
import functools
import math

import jax
import jax.numpy as jnp
from jax import lax
from jax.experimental import pallas as pl
from jax.experimental.pallas import tpu as pltpu
from jax.sharding import PartitionSpec as P

WIDTH = 128
NEG = -1e30
TINY = 1.2e-38


def kernel(
    dims,
    pairing_hbm,
    placement_hbm,
    scale_hbm,
    tq_hbm,
    tk_hbm,
    sq_hbm,
    sk_hbm,
    qg,
    kg,
    kl_ref,
    sg_ref,
    tq,
    tk,
    sq,
    sk,
    p_s,
    lp_s,
    g_s,
    rows_s,
    red_dp,
    red_head,
    pairing,
    placement,
    scale,
    in_sem,
    x_send,
    x_recv,
    s_send,
    s_recv,
    rd_send,
    rd_recv,
    rh_send,
    rh_recv,
    *gathered,
):
    n, n_head, n_dp, tokens, heads, groups, slots, layers = dims
    chunks = heads // 2
    per_group = heads // groups
    inverse = 1.0 / math.sqrt(WIDTH)
    me = lax.axis_index("section")
    my_head = lax.axis_index("head")
    my_dp = lax.axis_index("dp")
    half = n // 2
    sibling = me + 1 - 2 * lax.rem(me, 2)

    def lanes(index):
        return slice(index * WIDTH, (index + 1) * WIDTH)

    loads_t = [pltpu.make_async_copy(tk_hbm.at[0], tk, in_sem.at[0])]
    for c in range(chunks):
        part = slice(c * 4 * WIDTH, (c + 1) * 4 * WIDTH)
        loads_t.append(
            pltpu.make_async_copy(tq_hbm.at[0, :, part], tq.at[:, part], in_sem.at[3 + c])
        )
    loads_small = [
        pltpu.make_async_copy(pairing_hbm, pairing, in_sem.at[3 + chunks]),
        pltpu.make_async_copy(placement_hbm, placement, in_sem.at[4 + chunks]),
        pltpu.make_async_copy(scale_hbm, scale, in_sem.at[5 + chunks]),
    ]
    loads_s = [
        pltpu.make_async_copy(sk_hbm.at[0], sk, in_sem.at[1]),
        pltpu.make_async_copy(sq_hbm.at[0], sq, in_sem.at[2]),
    ]
    for copy in loads_t + loads_small + loads_s:
        copy.start()

    barrier = pltpu.get_barrier_semaphore()
    dp_peers = [
        ({"section": lax.rem(me + k, n), "dp": lax.rem(my_dp + d, n_dp)}, (k, d))
        for d in range(n_dp)
        for k in range(n)
        if (k, d) != (0, 0)
    ]
    head_peers = [
        ({"section": lax.rem(me + k, n), "head": lax.rem(my_head + h, n_head)}, (k, h))
        for h in range(1, n_head)
        for k in range(n)
    ]
    for peer, _ in dp_peers + head_peers:
        pl.semaphore_signal(barrier, inc=1, device_id=peer, device_id_type=pl.DeviceIdType.MESH)
    peers = len(dp_peers) + len(head_peers)

    def send(src, dst, send_sem, recv_sem, peer):
        return pltpu.make_async_remote_copy(
            src_ref=src,
            dst_ref=dst,
            send_sem=send_sem,
            recv_sem=recv_sem,
            device_id=peer,
            device_id_type=pl.DeviceIdType.MESH,
        )

    def remote(src, dst, send_sem, recv_sem, peer):
        return send(src, dst, send_sem, recv_sem, {"section": peer})

    key_ids = lax.broadcasted_iota(jnp.int32, (tokens, tokens), 0)
    query_ids = lax.broadcasted_iota(jnp.int32, (tokens, tokens), 1)
    visible = key_ids <= query_ids
    strict = key_ids < query_ids
    eye = key_ids == query_ids

    def nt(a, b):
        return lax.dot_general(a, b, (((1,), (1,)), ((), ())), preferred_element_type=jnp.float32)

    def target(key, b):
        total = None
        for a in (2 * b, 2 * b + 1):
            s = jnp.where(visible, nt(key, tq[:, lanes(a)]) * inverse, NEG)
            e = jnp.exp(s - jnp.max(s, axis=0, keepdims=True))
            p = e * (0.5 / jnp.sum(e, axis=0, keepdims=True))
            total = p if total is None else total + p
        return total

    entropy = jnp.zeros((1, tokens), jnp.float32)
    x_copies, s_copies = [], []
    loads_t[0].wait()
    for c in range(chunks):
        loads_t[1 + c].wait()
        buffer = gathered[c]
        b = 2 * c
        first = target(tk[:, lanes(b // per_group)], b)
        second = target(tk[:, lanes((b + 1) // per_group)], b + 1)
        buffer[me, :tokens, :] = jnp.where(visible, first, second.T)
        diagonal = jnp.sum(jnp.where(eye, second, 0.0), axis=0, keepdims=True)
        buffer[me, tokens:, :] = jnp.broadcast_to(diagonal, (8, tokens))
        for t in (first, second):
            entropy = entropy + jnp.sum(t * jnp.log(jnp.maximum(t, TINY)), axis=0, keepdims=True)
        if c == 0:
            pl.semaphore_wait(barrier, peers)
        mine = buffer.at[me, : tokens + 1]
        for k in range(1, half):
            copy = remote(
                mine, mine, x_send.at[c, k], x_recv.at[c, k], lax.rem(me + 2 * k, n)
            )
            copy.start()
            x_copies.append(copy)
        copy = remote(mine, mine, s_send.at[c, 0], s_recv.at[c, 0], sibling)
        copy.start()
        s_copies.append(copy)

    for copy in loads_small:
        copy.wait()

    count = jnp.int32(0)
    slot_layer = [jnp.int32(0)] * slots
    slot_teacher = [jnp.int32(0)] * slots
    taught = jnp.int32(0)
    for l in range(layers):
        held = placement[l] == me
        for j in range(slots):
            here = held & (count == j)
            slot_layer[j] = jnp.where(here, l, slot_layer[j])
            slot_teacher[j] = jnp.where(here, pairing[l], slot_teacher[j])
        count = count + held.astype(jnp.int32)
        taught = jnp.where(pairing[l] == me, l, taught)
    slot_valid = [count > j for j in range(slots)]

    def student(j, b):
        value = scale[slot_layer[j], b]
        raw = nt(sk[j, :, lanes(b // per_group)], sq[j, :, lanes(b)])
        z = jnp.where(visible, raw * (value * inverse), NEG)
        z = z - jnp.max(z, axis=0, keepdims=True)
        e = jnp.exp(z)
        l = jnp.sum(e, axis=0, keepdims=True)
        logp = z - jnp.log(l)
        p = e * (1.0 / l)
        p_s[j, b] = p
        lp_s[j, b] = logp
        rows_s[j, b : b + 1, :] = jnp.sum(p * logp, axis=0, keepdims=True)

    cross = [jnp.zeros((1, tokens), jnp.float32)] * slots

    def compare(c):
        for k in range(half):
            index = c if k == 0 else chunks + c * (half - 1) + k - 1
            s_copies[index].wait_recv()
        for j in range(slots):
            packed = gathered[c][slot_teacher[j], :tokens, :]
            diagonal = gathered[c][slot_teacher[j], tokens : tokens + 1, :]
            for b in (2 * c, 2 * c + 1):
                if b == 2 * c:
                    t = jnp.where(visible, packed, 0.0)
                else:
                    t = jnp.where(strict, packed.T, jnp.where(eye, diagonal, 0.0))
                value = scale[slot_layer[j], b]
                row = jnp.sum(t * lp_s[j, b], axis=0, keepdims=True)
                cross[j] = cross[j] + row
                spot = slice(b, b + 1)
                rows_s[j, spot, :] = (rows_s[j, spot, :] - row) / value
                factor = jnp.where(slot_valid[j], value * inverse, 0.0)
                g_s[j, b] = ((p_s[j, b] - t) * factor).astype(jnp.bfloat16)

    def gradients(j, g):
        key = sk[j, :, lanes(g)]
        total = None
        for b in range(g * per_group, (g + 1) * per_group):
            grad = g_s[j, b]
            qg[0, j, :, lanes(b)] = lax.dot_general(
                grad, key, (((0,), (0,)), ((), ())), preferred_element_type=jnp.float32
            ).astype(jnp.bfloat16)
            term = jnp.dot(grad, sq[j, :, lanes(b)], preferred_element_type=jnp.float32)
            total = term if total is None else total + term
        kg[0, j, :, lanes(g)] = total.astype(jnp.bfloat16)

    ready = 0

    def finished_groups(heads_done, first):
        last = heads_done // per_group
        for g in range(first, last):
            for j in range(slots):
                gradients(j, g)
        return last

    for copy in loads_s:
        copy.wait()
    for c in range(chunks):
        for j in range(slots):
            for b in (2 * c, 2 * c + 1):
                student(j, b)
        for k in range(1, half):
            x_copies[c * (half - 1) + k - 1].wait_recv()
            block = gathered[c].at[lax.rem(me + n - 2 * k, n), : tokens + 1]
            copy = remote(block, block, s_send.at[c, k], s_recv.at[c, k], sibling)
            copy.start()
            s_copies.append(copy)
        if c > 0:
            ready = finished_groups(2 * (c - 1), ready)
            compare(c - 1)
    ready = finished_groups(2 * (chunks - 1), ready)
    compare(chunks - 1)

    tile_rows = red_dp.shape[2]
    row_ids = lax.broadcasted_iota(jnp.int32, (tile_rows, WIDTH), 0)
    lane_ids = lax.broadcasted_iota(jnp.int32, (tile_rows, WIDTH), 1)
    head_rows = lax.broadcasted_iota(jnp.int32, (heads, WIDTH), 0)
    head_lanes = lax.broadcasted_iota(jnp.int32, (heads, WIDTH), 1)
    tile = jnp.where(
        (row_ids == taught) & (lane_ids == heads), jnp.sum(entropy, axis=1, keepdims=True), 0.0
    )
    for j in range(slots):
        column = jnp.sum(rows_s[j], axis=1, keepdims=True)
        line = jnp.sum(jnp.where(head_rows == head_lanes, column, 0.0), axis=0, keepdims=True)
        line = jnp.where(lane_ids == heads, -jnp.sum(cross[j], axis=1, keepdims=True), line)
        owner = jnp.where(slot_valid[j], slot_layer[j], -1)
        tile = tile + jnp.where(row_ids == owner, line, 0.0)
    red_dp[me, my_dp] = tile
    mine = red_dp.at[me, my_dp]
    r_copies = []
    for peer, (k, h) in head_peers:
        r_copies.append(
            send(mine, red_head.at[me, my_head], rh_send.at[k, h], rh_recv.at[k, h], peer)
        )
    for peer, (k, d) in dp_peers:
        r_copies.append(send(mine, mine, rd_send.at[k, d], rd_recv.at[k, d], peer))
    for copy in r_copies:
        copy.start()

    finished_groups(heads, ready)

    for copy in r_copies:
        copy.wait_recv()
    for s in range(n):
        red_head[s, my_head] = red_dp[s, my_dp]

    def added(buffer, size):
        total = None
        for a in range(size):
            for s in range(n):
                total = buffer[s, a] if total is None else total + buffer[s, a]
        return total

    sg_ref[...] = added(red_dp, n_dp)[:layers, :heads]
    column = jnp.sum(
        jnp.where(lane_ids == heads, added(red_head, n_head), 0.0), axis=1, keepdims=True
    )
    line = jnp.sum(jnp.where(row_ids == lane_ids, column, 0.0), axis=0, keepdims=True)
    kl_ref[...] = (line / (heads * n_head * tokens))[:, :layers]

    for copy in x_copies + s_copies + r_copies:
        copy.wait_send()


def hand_out(*refs):
    count = len(refs) // 2
    sems = refs[-1]
    copies = [
        pltpu.make_async_copy(refs[i], refs[count + i], sems.at[i]) for i in range(count)
    ]
    for copy in copies:
        copy.start()
    for copy in copies:
        copy.wait()


def local(n, n_head, n_dp, teacher_q, teacher_k, student_q, student_k, student_scale, pairing, placement):
    layers, heads = student_scale.shape
    slots, tokens = student_q.shape[1:3]
    groups = student_k.shape[3] // WIDTH
    chunks = heads // 2
    tile_rows = -(-layers // 8) * 8
    dims = (n, n_head, n_dp, tokens, heads, groups, slots, layers)
    hbm = pl.BlockSpec(memory_space=pltpu.HBM)
    vmem = pl.BlockSpec(memory_space=pltpu.VMEM)
    dma = pltpu.SemaphoreType.DMA
    f32, bf16 = jnp.float32, jnp.bfloat16
    shapes = (
        (student_q.shape, bf16),
        (student_k.shape, bf16),
        ((1, layers), f32),
        ((layers, heads), f32),
    )
    results = pl.pallas_call(
        functools.partial(kernel, dims),
        out_shape=tuple(pltpu.VMEM(*shape) for shape in shapes),
        in_specs=[hbm] * 7,
        out_specs=(vmem,) * 4,
        scratch_shapes=[
            pltpu.VMEM(teacher_q.shape[1:], bf16),
            pltpu.VMEM(teacher_k.shape[1:], bf16),
            pltpu.VMEM(student_q.shape[1:], bf16),
            pltpu.VMEM(student_k.shape[1:], bf16),
            pltpu.VMEM((slots, heads, tokens, tokens), f32),
            pltpu.VMEM((slots, heads, tokens, tokens), f32),
            pltpu.VMEM((slots, heads, tokens, tokens), bf16),
            pltpu.VMEM((slots, heads, tokens), f32),
            pltpu.VMEM((n, n_dp, tile_rows, WIDTH), f32),
            pltpu.VMEM((n, n_head, tile_rows, WIDTH), f32),
            pltpu.SMEM(pairing.shape, jnp.int32),
            pltpu.SMEM(placement.shape, jnp.int32),
            pltpu.SMEM(student_scale.shape, f32),
            dma((6 + chunks,)),
            dma((chunks, n // 2)),
            dma((chunks, n // 2)),
            dma((chunks, n // 2)),
            dma((chunks, n // 2)),
            dma((n, n_dp)),
            dma((n, n_dp)),
            dma((n, n_head)),
            dma((n, n_head)),
        ]
        + [pltpu.VMEM((n, tokens + 8, tokens), f32) for _ in range(chunks)],
        compiler_params=pltpu.CompilerParams(
            collective_id=0, has_side_effects=True, vmem_limit_bytes=56 * 1024 * 1024
        ),
    )(pairing, placement, student_scale, teacher_q, teacher_k, student_q, student_k)
    return pl.pallas_call(
        hand_out,
        out_shape=tuple(jax.ShapeDtypeStruct(*shape) for shape in shapes),
        in_specs=[vmem] * 4,
        out_specs=(hbm,) * 4,
        scratch_shapes=[dma((4,))],
        compiler_params=pltpu.CompilerParams(vmem_limit_bytes=4 * 1024 * 1024),
    )(*results)


def solution(mesh):
    sizes = (mesh.shape["section"], mesh.shape["head"], mesh.shape["dp"])
    return jax.shard_map(
        functools.partial(local, *sizes),
        mesh=mesh,
        in_specs=(
            P("section", "dp", "head"),
            P("section", "dp", "head"),
            P("section", None, "dp", "head"),
            P("section", None, "dp", "head"),
            P(None, "head"),
            P(),
            P(),
        ),
        out_specs=(
            P("section", None, "dp", "head"),
            P("section", None, "dp", "head"),
            P("dp", None),
            P(None, "head"),
        ),
        check_vma=False,
    )
```
